32 devices in a mesh: fsdp: 8 (over z, core), cols: 4 (over y, x).
Axes of the slice: x: 2, y: 2, z: 4, core: 2. Of those that a mesh axis runs over, the one named last changes fastest.
Arguments:
- one_query: float32 [4096, 4096], P('fsdp', 'cols'), may hold values from -0.125 to 0.125
- other_query: float32 [4096, 4096], P('fsdp', 'cols'), may hold values from -0.09375 to 0.09375
- one_key: float32 [4096, 4096], P('fsdp', 'cols'), may hold values from -0.125 to 0.125
- other_key: float32 [4096, 4096], P('fsdp', 'cols'), may hold values from -0.09375 to 0.09375
- one_value: float32 [4096, 4096], P('fsdp', 'cols'), may hold values from -0.125 to 0.125
- other_value: float32 [4096, 4096], P('fsdp', 'cols'), may hold values from -0.09375 to 0.09375
- mix_share: float32 [4096], P('fsdp'), may hold values from 0.2 to 0.8
- norm_train: float32 [4096], P(('fsdp', 'cols')), may hold values from 0.25 to 1.75
- norm_step: float32 [4096], P(('fsdp', 'cols')), may hold values from -0.3 to 0.3
Outputs:
- final_query: bfloat16 [4096, 4096], P(None, 'cols')
- final_key: bfloat16 [4096, 4096], P(None, 'cols')
- final_value: bfloat16 [4096, 4096], P(None, 'cols')
- scale_query: float32 [4096], P('cols')
- scale_key: float32 [4096], P('cols')
- scale_value: float32 [4096], P('cols')
- serve_norm: bfloat16 [4096], replicated
The draws below stay inside these ranges and needn't reach their ends.
All inputs are finite; a program needn't handle non-finite values.
Results may differ from the reference program's by a relative error of at most 0.0004.
Values may be sent and summed in bfloat16 or wider, within the bound.
No kernel may reach another device: no remote copies, remote signals or barrier semaphores. Data moves between devices by JAX's collectives and lax.ppermute only.
A program may use at most 128 MiB of HBM per device.

```python
import jax
import jax.numpy as jnp
from jax import lax

D_MODEL = 4096
Q_DIM = 4096
KV_DIM = 4096


def with_spikes(values, stream_key, source, target, shards_of, factor):
    owner, partner = [(jnp.arange(values.shape[position]) // (values.shape[position] // shards_of)).reshape([-1 if axis == position else 1 for axis in range(values.ndim)]) for position in (source, target)]
    chosen = jax.random.permutation(stream_key, shards_of)[partner]
    strong = (owner == chosen) | (owner == (partner + shards_of // 2) % shards_of)
    return jnp.where(strong, factor * values, values)


def level_of(rng, extent, split, low, top_value):
    loudness = 1.0
    for position, parts in split:
        steps = jax.random.uniform(jax.random.fold_in(jax.random.fold_in(rng, 6), position), (parts,), jnp.float32, low / len(split), top_value / len(split))
        loudness = loudness * jnp.repeat(jnp.exp(steps), extent[position] // parts).reshape((-1,) + (1,) * (len(extent) - 1 - position))
    return loudness


def noise(stream_key, dims, deviation, limit, shards=(), held_as=jnp.bfloat16):
    factor_of = level_of(stream_key, dims, shards, -0.22, 0.18) if shards else 1.0
    drawn = jax.random.normal(stream_key, dims, jnp.float32) * deviation * factor_of
    return jnp.minimum(jnp.maximum(drawn, -limit), limit).astype(held_as)


def gaussian_with(stream_key, dims, scale, most, cuts, heavy, dtype=jnp.bfloat16):
    values = scale * jax.random.normal(stream_key, dims, jnp.float32)
    if cuts:
        values = values * level_of(stream_key, dims, cuts, -0.22, 0.18)
    return jnp.clip(with_spikes(values, jax.random.fold_in(stream_key, 3), *heavy), -most, most).astype(dtype)


def setup_inputs(seed: int = 0) -> dict:
    key_list = jax.random.split(jax.random.key(seed), 10)
    one_query = gaussian_with(key_list[0], (D_MODEL, Q_DIM), D_MODEL ** -0.5, 0.125, ((0, 8), (1, 4)), (0, 1, 8, 2.0), jnp.float32)
    other_query = noise(key_list[1], (D_MODEL, Q_DIM), D_MODEL ** -0.5, 0.09375, ((0, 8), (1, 4)), jnp.float32)
    one_key = gaussian_with(key_list[2], (D_MODEL, KV_DIM), D_MODEL ** -0.5, 0.125, ((0, 8), (1, 4)), (0, 1, 8, 2.0), jnp.float32)
    other_key = noise(key_list[3], (D_MODEL, KV_DIM), D_MODEL ** -0.5, 0.09375, ((0, 8), (1, 4)), jnp.float32)
    one_value = gaussian_with(key_list[4], (D_MODEL, KV_DIM), D_MODEL ** -0.5, 0.125, ((0, 8), (1, 4)), (0, 1, 8, 2.0), jnp.float32)
    other_value = noise(key_list[5], (D_MODEL, KV_DIM), D_MODEL ** -0.5, 0.09375, ((0, 8), (1, 4)), jnp.float32)
    mix_share = jnp.clip(0.2 + 0.6 * jax.random.uniform(key_list[6], (D_MODEL,), jnp.float32) ** level_of(key_list[6], (D_MODEL,), ((0, 8),), -0.2, 0.2), 0.2, 0.8)
    norm_train = jnp.clip(1.0 + 0.15 * jax.random.normal(key_list[7], (D_MODEL,), jnp.float32), 0.25, 1.75)
    norm_step = jnp.clip(jax.random.uniform(key_list[8], (D_MODEL,), jnp.float32, -0.3, 0.3) * level_of(key_list[8], (D_MODEL,), ((0, 32),), -0.4, 0.0), -0.3, 0.3)
    return dict(one_query=one_query, other_query=other_query, one_key=one_key, other_key=other_key, one_value=one_value, other_value=other_value, mix_share=mix_share, norm_train=norm_train, norm_step=norm_step)


def reference(one_query, other_query, one_key, other_key, one_value, other_value, mix_share, norm_train, norm_step):
    result_query = mix_share[:, None] * one_query + (1.0 - mix_share[:, None]) * other_query
    result_key = mix_share[:, None] * one_key + (1.0 - mix_share[:, None]) * other_key
    result_value = mix_share[:, None] * one_value + (1.0 - mix_share[:, None]) * other_value
    scale_query = jnp.sqrt(lax.optimization_barrier(jnp.sum(result_query * result_query, axis=0)))
    final_query = (result_query / scale_query).astype(jnp.bfloat16)
    scale_key = jnp.sqrt(lax.optimization_barrier(jnp.sum(result_key * result_key, axis=0)))
    final_key = (result_key / scale_key).astype(jnp.bfloat16)
    scale_value = jnp.sqrt(lax.optimization_barrier(jnp.sum(result_value * result_value, axis=0)))
    final_value = (result_value / scale_value).astype(jnp.bfloat16)
    serve_norm = (norm_train + norm_step).astype(jnp.bfloat16)
    return (final_query, final_key, final_value, scale_query, scale_key, scale_value, serve_norm)
```

```python
import functools

import jax
import jax.numpy as jnp
from jax import lax
from jax.experimental import pallas as pl
from jax.experimental.pallas import tpu as pltpu
from jax.sharding import PartitionSpec as P


NEAR = ((0, 1), (1, 0), (2, 3), (3, 2))
MID = ((1, 2), (2, 1))
EDGE = ((1, 0), (2, 3))
ALL = (0, 1, 2, 3)
INNER = (1, 2)
OUTER = (0, 3)


def lanes(pairs):
    return [(2 * s + c, 2 * d + c) for s, d in pairs for c in (0, 1)]


def partners(chips):
    return [(2 * z + c, 2 * z + 1 - c) for z in chips for c in (0, 1)]


def along(x, pairs):
    return lax.ppermute(x, "fsdp", lanes(pairs))


def across(x, chips):
    return lax.ppermute(x, "fsdp", partners(chips))


def place(at, parts, whole, total):
    names = [p[2] for p in parts]
    blocks = [b for p in parts for b in p[:2]]
    rows, width = blocks[0].shape
    cuts = 2
    step = rows // cuts

    def kernel(at_ref, *refs):
        block_refs = refs[: len(blocks)]
        out = refs[-2]
        sems = refs[-1]
        z = at_ref[0]
        core = at_ref[1]
        for zi in ALL:
            inner = zi in INNER
            where = {"own": zi, "near": zi ^ 1}
            if inner:
                where.update(mid=3 - zi, far=3 - (zi ^ 1))
            else:
                where.update(edge=3 - (zi ^ 1), last=3 - zi)
            for ci in (0, 1):

                @pl.when((z == zi) & (core == ci))
                def _():
                    copies = []
                    for k, name in enumerate(names):
                        if name not in where:
                            continue
                        for lane in (0, 1):
                            src = block_refs[2 * k + (0 if lane == ci else 1)]
                            base = (where[name] * 2 + lane) * rows
                            for h in range(cuts):
                                copies.append(
                                    pltpu.make_async_copy(
                                        src.at[pl.ds(h * step, step)],
                                        out.at[pl.ds(base + h * step, step)],
                                        sems.at[len(copies)],
                                    )
                                )
                    for c in copies:
                        c.start()
                    for c in copies:
                        c.wait()

    any_spec = pl.BlockSpec(memory_space=pl.ANY)
    args = [at, *blocks]
    aliases = {}
    if whole is not None:
        aliases = {len(args): 0}
        args.append(whole)
    return pl.pallas_call(
        kernel,
        in_specs=[pl.BlockSpec(memory_space=pltpu.SMEM)] + [any_spec] * (len(args) - 1),
        out_specs=any_spec,
        out_shape=jax.ShapeDtypeStruct((total, width), blocks[0].dtype),
        scratch_shapes=[pltpu.SemaphoreType.DMA((2 * cuts * len(names),))],
        input_output_aliases=aliases,
    )(*args)


def line_gathers(narrows):
    n = range(len(narrows))
    member = lax.axis_index("fsdp")
    at = jnp.stack([member // 2, member % 2]).astype(jnp.int32)
    total = narrows[0].shape[0] * 8
    near = [along(x, NEAR) for x in narrows]
    mid = [along(x, MID) for x in narrows]
    own_p = [across(x, ALL) for x in narrows]
    edge = [along(x, EDGE) for x in mid]
    far = [along(x, MID) for x in near]
    near_p = [across(x, ALL) for x in near]
    mid_p = [across(x, INNER) for x in mid]
    last = [along(x, EDGE) for x in far]
    edge_p = [across(x, OUTER) for x in edge]
    far_p = [across(x, INNER) for x in far]
    last_p = [across(x, OUTER) for x in last]
    outs = []
    for i in n:
        early = (
            (narrows[i], own_p[i], "own"),
            (near[i], near_p[i], "near"),
            (mid[i], mid_p[i], "mid"),
            (edge[i], edge_p[i], "edge"),
        )
        late = ((far[i], far_p[i], "far"), (last[i], last_p[i], "last"))
        whole = place(at, early, None, total)
        outs.append(place(at, late, whole, total))
    return outs


def pair_sums(x, axis, size):
    bit = 1
    while bit < size:
        x = x + lax.ppermute(x, axis, [(k, k ^ bit) for k in range(size)])
        bit *= 2
    return x


def per_device(sizes, *args):
    *weights, mix_share, norm_train, norm_step = args
    fsdp, cols = sizes
    share = mix_share[:, None]
    mixed = lambda k: share * weights[2 * k] + (1.0 - share) * weights[2 * k + 1]
    width = weights[0].shape[1]
    sums = [jnp.sum(jnp.square(mixed(k)), axis=0) for k in range(3)]
    gain = (norm_train + norm_step).astype(jnp.bfloat16)
    piece = gain.shape[0]
    line = fsdp == 8 and cols & (cols - 1) == 0

    if line:
        slot = lax.dynamic_update_slice(
            jnp.zeros((fsdp * piece,), jnp.float32),
            gain.astype(jnp.float32),
            (lax.axis_index("fsdp") * piece,),
        )
        both = pair_sums(jnp.concatenate(sums + [slot]), "fsdp", fsdp)
        totals = [both[k * width : (k + 1) * width] for k in range(3)]
        slot = both[3 * width :].reshape(fsdp, 1, piece).astype(jnp.bfloat16)
    else:
        totals = lax.psum(tuple(sums), "fsdp")
    scales = [jnp.sqrt(t) for t in totals]
    if not line:
        narrows = [(mixed(k) / scales[k]).astype(jnp.bfloat16) for k in range(3)]
        finals = [lax.all_gather(x, "fsdp", axis=0, tiled=True) for x in narrows]
        serve = lax.all_gather(gain, ("fsdp", "cols"), axis=0, tiled=True)
        return (*finals, *scales, serve)
    narrows = [(mixed(k) / scales[k]).astype(jnp.bfloat16) for k in range(3)]
    finals = line_gathers(narrows)
    serve = lax.dynamic_update_slice(
        jnp.zeros((fsdp, cols, piece), jnp.bfloat16), slot, (0, lax.axis_index("cols"), 0)
    )
    serve = pair_sums(serve, "cols", cols).reshape(-1)
    return (*finals, *scales, serve)


def solution(mesh):
    sizes = (mesh.shape["fsdp"], mesh.shape["cols"])
    weight = P("fsdp", "cols")
    gain = P(("fsdp", "cols"))
    return jax.shard_map(
        functools.partial(per_device, sizes),
        mesh=mesh,
        in_specs=(weight,) * 6 + (P("fsdp"), gain, gain),
        out_specs=(P(None, "cols"),) * 3 + (P("cols"),) * 3 + (P(),),
        check_vma=False,
    )
```

```python
import functools

import jax
import jax.numpy as jnp
from jax import lax
from jax.experimental import pallas as pl
from jax.experimental.pallas import tpu as pltpu
from jax.sharding import PartitionSpec as P


NEAR = ((0, 1), (1, 0), (2, 3), (3, 2))
MID = ((1, 2), (2, 1))
EDGE = ((1, 0), (2, 3))
ALL = (0, 1, 2, 3)
INNER = (1, 2)
OUTER = (0, 3)


def lanes(pairs):
    return [(2 * s + c, 2 * d + c) for s, d in pairs for c in (0, 1)]


def partners(chips):
    return [(2 * z + c, 2 * z + 1 - c) for z in chips for c in (0, 1)]


def along(x, pairs):
    return lax.ppermute(x, "fsdp", lanes(pairs))


def across(x, chips):
    return lax.ppermute(x, "fsdp", partners(chips))


def place(at, parts, whole, total):
    names = [p[2] for p in parts]
    blocks = [b for p in parts for b in p[:2]]
    rows, width = blocks[0].shape
    cuts = 2
    step = rows // cuts

    def kernel(at_ref, *refs):
        block_refs = refs[: len(blocks)]
        out, held, arrived, left = refs[-4:]
        z = at_ref[0]
        core = at_ref[1]
        for zi in ALL:
            inner = zi in INNER
            where = {"own": zi, "near": zi ^ 1}
            if inner:
                where.update(mid=3 - zi, far=3 - (zi ^ 1))
            else:
                where.update(edge=3 - (zi ^ 1), last=3 - zi)
            for ci in (0, 1):

                @pl.when((z == zi) & (core == ci))
                def _():
                    loads = []
                    stores = []
                    for k, name in enumerate(names):
                        if name not in where:
                            continue
                        for lane in (0, 1):
                            src = block_refs[2 * k + (0 if lane == ci else 1)]
                            base = (where[name] * 2 + lane) * rows
                            for h in range(cuts):
                                j = len(loads)
                                room = held.at[pl.ds(j * step, step)]
                                loads.append(
                                    pltpu.make_async_copy(
                                        src.at[pl.ds(h * step, step)], room, arrived.at[j]
                                    )
                                )
                                stores.append(
                                    pltpu.make_async_copy(
                                        room, out.at[pl.ds(base + h * step, step)], left.at[j]
                                    )
                                )
                    for c in loads:
                        c.start()
                    for c, d in zip(loads, stores):
                        c.wait()
                        d.start()
                    for d in stores:
                        d.wait()

    hbm = pl.BlockSpec(memory_space=pltpu.HBM)
    args = [at, *blocks]
    aliases = {}
    if whole is not None:
        aliases = {len(args): 0}
        args.append(whole)
    slots = 2 * cuts * len(names)
    return pl.pallas_call(
        kernel,
        in_specs=[pl.BlockSpec(memory_space=pltpu.SMEM)] + [hbm] * (len(args) - 1),
        out_specs=hbm,
        out_shape=jax.ShapeDtypeStruct((total, width), blocks[0].dtype),
        scratch_shapes=[
            pltpu.VMEM((slots * step, width), blocks[0].dtype),
            pltpu.SemaphoreType.DMA((slots,)),
            pltpu.SemaphoreType.DMA((slots,)),
        ],
        input_output_aliases=aliases,
    )(*args)


def line_gathers(narrows):
    n = range(len(narrows))
    member = lax.axis_index("fsdp")
    at = jnp.stack([member // 2, member % 2]).astype(jnp.int32)
    total = narrows[0].shape[0] * 8
    near = [along(x, NEAR) for x in narrows]
    mid = [along(x, MID) for x in narrows]
    own_p = [across(x, ALL) for x in narrows]
    edge = [along(x, EDGE) for x in mid]
    far = [along(x, MID) for x in near]
    near_p = [across(x, ALL) for x in near]
    mid_p = [across(x, INNER) for x in mid]
    edge_p = [across(x, OUTER) for x in edge]
    wholes = []
    for i in n:
        early = (
            (narrows[i], own_p[i], "own"),
            (near[i], near_p[i], "near"),
            (mid[i], mid_p[i], "mid"),
            (edge[i], edge_p[i], "edge"),
        )
        with jax.named_scope(f"early{i}"):
            wholes.append(place(at, early, None, total))
    *wholes, far[-1] = lax.optimization_barrier((*wholes, far[-1]))
    last = []
    for i in n:
        with jax.named_scope(f"last{i}"):
            last.append(along(far[i], EDGE))
    far_p = [across(x, INNER) for x in far]
    last_p = [across(x, OUTER) for x in last]
    outs = []
    for i in n:
        late = ((far[i], far_p[i], "far"), (last[i], last_p[i], "last"))
        with jax.named_scope(f"late{i}"):
            outs.append(place(at, late, wholes[i], total))
    return outs


def pair_sums(x, axis, size):
    bit = 1
    while bit < size:
        x = x + lax.ppermute(x, axis, [(k, k ^ bit) for k in range(size)])
        bit *= 2
    return x


def per_device(sizes, *args):
    *weights, mix_share, norm_train, norm_step = args
    fsdp, cols = sizes
    width = weights[0].shape[1]
    gain = (norm_train + norm_step).astype(jnp.bfloat16)
    piece = gain.shape[0]

    def mixed(k, share):
        share = share[:, None]
        return share * weights[2 * k] + (1.0 - share) * weights[2 * k + 1]

    def power_sum(k, share):
        return jnp.sum(jnp.square(mixed(k, share)), axis=0)

    def narrow(k, share, scale):
        return (mixed(k, share) / scale).astype(jnp.bfloat16)

    if fsdp != 8 or cols & (cols - 1) != 0:
        totals = lax.psum(tuple(power_sum(k, mix_share) for k in range(3)), "fsdp")
        scales = [jnp.sqrt(t) for t in totals]
        narrows = [narrow(k, mix_share, scales[k]) for k in range(3)]
        finals = [lax.all_gather(x, "fsdp", axis=0, tiled=True) for x in narrows]
        serve = lax.all_gather(gain, ("fsdp", "cols"), axis=0, tiled=True)
        return (*finals, *scales, serve)

    first = power_sum(0, mix_share)
    share, first = lax.optimization_barrier((mix_share, first))
    total = pair_sums(first, "fsdp", fsdp)
    slot = lax.dynamic_update_slice(
        jnp.zeros((fsdp * piece,), jnp.float32),
        gain.astype(jnp.float32),
        (lax.axis_index("fsdp") * piece,),
    )
    rest = jnp.concatenate([power_sum(1, share), power_sum(2, share), slot])
    scale = jnp.sqrt(total)
    block = narrow(0, mix_share, scale)
    rest, block = lax.optimization_barrier((rest, block))
    rest = pair_sums(rest, "fsdp", fsdp)
    scales = [scale, jnp.sqrt(rest[:width]), jnp.sqrt(rest[width : 2 * width])]
    slot = rest[2 * width :].reshape(fsdp, 1, piece).astype(jnp.bfloat16)
    narrows = [block] + [narrow(k, share, scales[k]) for k in (1, 2)]
    finals = line_gathers(narrows)
    serve = lax.dynamic_update_slice(
        jnp.zeros((fsdp, cols, piece), jnp.bfloat16), slot, (0, lax.axis_index("cols"), 0)
    )
    serve = pair_sums(serve, "cols", cols).reshape(-1)
    return (*finals, *scales, serve)


def solution(mesh):
    sizes = (mesh.shape["fsdp"], mesh.shape["cols"])
    weight = P("fsdp", "cols")
    gain = P(("fsdp", "cols"))
    return jax.shard_map(
        functools.partial(per_device, sizes),
        mesh=mesh,
        in_specs=(weight,) * 6 + (P("fsdp"), gain, gain),
        out_specs=(P(None, "cols"),) * 3 + (P("cols"),) * 3 + (P(),),
        check_vma=False,
    )
```

```python
import functools

import jax
import jax.numpy as jnp
from jax import lax
from jax.experimental import pallas as pl
from jax.experimental.pallas import tpu as pltpu
from jax.sharding import PartitionSpec as P


NEAR = ((0, 1), (1, 0), (2, 3), (3, 2))
MID = ((1, 2), (2, 1))
EDGE = ((1, 0), (2, 3))
ALL = (0, 1, 2, 3)
INNER = (1, 2)
OUTER = (0, 3)


def lanes(pairs):
    return [(2 * s + c, 2 * d + c) for s, d in pairs for c in (0, 1)]


def partners(chips):
    return [(2 * z + c, 2 * z + 1 - c) for z in chips for c in (0, 1)]


def along(x, pairs):
    return lax.ppermute(x, "fsdp", lanes(pairs))


def across(x, chips):
    return lax.ppermute(x, "fsdp", partners(chips))


def place(at, parts, whole, total):
    names = [p[2] for p in parts]
    blocks = [b for p in parts for b in p[:2]]
    rows, width = blocks[0].shape
    cuts = 4
    step = rows // cuts

    def kernel(at_ref, *refs):
        block_refs = refs[: len(blocks)]
        out, held, arrived, left = refs[-4:]
        z = at_ref[0]
        core = at_ref[1]
        for zi in ALL:
            inner = zi in INNER
            where = {"own": zi, "near": zi ^ 1}
            if inner:
                where.update(mid=3 - zi, far=3 - (zi ^ 1))
            else:
                where.update(edge=3 - (zi ^ 1), last=3 - zi)
            for ci in (0, 1):

                @pl.when((z == zi) & (core == ci))
                def _():
                    loads = []
                    stores = []
                    for k, name in enumerate(names):
                        if name not in where:
                            continue
                        for lane in (0, 1):
                            src = block_refs[2 * k + (0 if lane == ci else 1)]
                            base = (where[name] * 2 + lane) * rows
                            for h in range(cuts):
                                j = len(loads)
                                room = held.at[pl.ds(j * step, step)]
                                loads.append(
                                    pltpu.make_async_copy(
                                        src.at[pl.ds(h * step, step)], room, arrived.at[j]
                                    )
                                )
                                stores.append(
                                    pltpu.make_async_copy(
                                        room, out.at[pl.ds(base + h * step, step)], left.at[j]
                                    )
                                )
                    for c in loads:
                        c.start()
                    for c, d in zip(loads, stores):
                        c.wait()
                        d.start()
                    for d in stores:
                        d.wait()

    hbm = pl.BlockSpec(memory_space=pltpu.HBM)
    args = [at, *blocks]
    aliases = {}
    if whole is not None:
        aliases = {len(args): 0}
        args.append(whole)
    slots = 2 * cuts * len(names)
    return pl.pallas_call(
        kernel,
        in_specs=[pl.BlockSpec(memory_space=pltpu.SMEM)] + [hbm] * (len(args) - 1),
        out_specs=hbm,
        out_shape=jax.ShapeDtypeStruct((total, width), blocks[0].dtype),
        scratch_shapes=[
            pltpu.VMEM((slots * step, width), blocks[0].dtype),
            pltpu.SemaphoreType.DMA((slots,)),
            pltpu.SemaphoreType.DMA((slots,)),
        ],
        input_output_aliases=aliases,
    )(*args)


def line_gathers(narrows):
    n = range(len(narrows))
    member = lax.axis_index("fsdp")
    at = jnp.stack([member // 2, member % 2]).astype(jnp.int32)
    total = narrows[0].shape[0] * 8

    def each(send, blocks, where):
        sent = []
        for i in n:
            sent.append(send(blocks[i], where))
        return sent

    near = each(along, narrows, NEAR)
    mid = each(along, narrows, MID)
    own_p = each(across, narrows, ALL)
    edge = each(along, mid, EDGE)
    far = each(along, near, MID)
    near_p = each(across, near, ALL)
    mid_p = each(across, mid, INNER)
    last = each(along, far, EDGE)
    edge_p = each(across, edge, OUTER)
    far_p = each(across, far, INNER)
    last_p = each(across, last, OUTER)
    outs = []
    for i in n:
        early = (
            (narrows[i], own_p[i], "own"),
            (near[i], near_p[i], "near"),
            (mid[i], mid_p[i], "mid"),
            (edge[i], edge_p[i], "edge"),
        )
        late = ((far[i], far_p[i], "far"), (last[i], last_p[i], "last"))
        whole = place(at, early, None, total)
        outs.append(place(at, late, whole, total))
    return outs


def pair_sums(x, axis, size):
    for step in range(size.bit_length() - 1):
        pairs = [(k, k ^ (1 << step)) for k in range(size)]
        got = lax.ppermute(x, axis, pairs)
        x = x + got
    return x


def on_line(fsdp, cols):
    return fsdp == 8 and cols == 4


def per_device(sizes, *args):
    *weights, mix_share, norm_train, norm_step = args
    fsdp, cols = sizes
    width = weights[0].shape[1]
    gain = (norm_train + norm_step).astype(jnp.bfloat16)
    piece = gain.shape[0]

    def mixed(k, share):
        share = share[:, None]
        return weights[2 * k + 1] + share * (weights[2 * k] - weights[2 * k + 1])

    def power_sum(k, share):
        return jnp.sum(jnp.square(mixed(k, share)), axis=0)

    def narrow(k, share, scale):
        return (mixed(k, share) / scale).astype(jnp.bfloat16)

    if not on_line(fsdp, cols):
        totals = lax.psum(tuple(power_sum(k, mix_share) for k in range(3)), "fsdp")
        scales = [jnp.sqrt(t) for t in totals]
        narrows = [narrow(k, mix_share, scales[k]) for k in range(3)]
        finals = [lax.all_gather(x, "fsdp", axis=0, tiled=True) for x in narrows]
        serve = lax.all_gather(gain, ("fsdp", "cols"), axis=0, tiled=True)
        return (*finals, *scales, serve)

    slot = lax.dynamic_update_slice(
        jnp.zeros((fsdp * piece,), jnp.float32),
        gain.astype(jnp.float32),
        (lax.axis_index("fsdp") * piece,),
    )
    sums = [power_sum(k, mix_share) for k in range(3)]
    both = pair_sums(jnp.concatenate(sums + [slot]), "fsdp", fsdp)
    scales = [jnp.sqrt(both[k * width : (k + 1) * width]) for k in range(3)]
    slot = both[3 * width :].reshape(fsdp, 1, piece).astype(jnp.bfloat16)
    block = narrow(0, mix_share, scales[0])
    share, block = lax.optimization_barrier((mix_share, block))
    narrows = [block] + [narrow(k, share, scales[k]) for k in (1, 2)]
    finals = line_gathers(narrows)
    serve = lax.dynamic_update_slice(
        jnp.zeros((fsdp, cols, piece), jnp.bfloat16), slot, (0, lax.axis_index("cols"), 0)
    )
    serve = pair_sums(serve, "cols", cols).reshape(-1)
    return (*finals, *scales, serve)


def solution(mesh):
    sizes = (mesh.shape["fsdp"], mesh.shape["cols"])
    weight = P("fsdp", "cols")
    gain = P(("fsdp", "cols"))
    return jax.shard_map(
        functools.partial(per_device, sizes),
        mesh=mesh,
        in_specs=(weight,) * 6 + (P("fsdp"), gain, gain),
        out_specs=(P(None, "cols"),) * 3 + (P("cols"),) * 3 + (P(),),
        check_vma=False,
    )
```
